256 devices in a mesh: tm: 64 (over z, y, core), freq: 4 (over x).
Axes of the slice: x: 4, y: 4, z: 8, core: 2. Of those that a mesh axis runs over, the one named last changes fastest.
Arguments:
- snapshots: bfloat16 [4352, 3, 32768], P('tm', None, 'freq'), may hold values from -200 to 200
- block_starts: int32 [32], replicated, may hold values from 0 to 4032, as said below
- freq_index: int32 [16], replicated, may hold values from 0 to 128
Outputs:
- modes: bfloat16 [16, 32, 2, 3, 32768], P(None, None, None, None, ('freq', 'tm'))
- energy: float32 [16], replicated
The draws below stay inside these ranges and needn't reach their ends.
Inputs may be any that keep to these rules, and one draw needn't show every extreme that they name: `block_starts`: block b starts at b * 128 plus between 0 and 64.
All inputs are finite; a program needn't handle non-finite values.
Results may differ from the reference program's by a relative error of at most 0.0085.
Values may be sent and summed in bfloat16 or wider, within the bound.
A program may use at most 64 MiB of HBM per device.

```python
import math
import jax
import jax.numpy as jnp
from jax import lax

NB = 32
NFFT = 256
NF = 16
HOP = 128
JIT = 64
TT = 4352
NSIT = 6
P_DEV = 128
P_SIZE = 32768


def draw_snapshots(key, part):
    key_noise, key_space, key_time = jax.random.split(key, 3)
    rising = jnp.exp(math.log(3.0) * jnp.arange(P_SIZE, dtype=jnp.float32) / P_SIZE)
    space_scale = rising * jnp.exp(jax.random.uniform(key_space, (P_SIZE,), minval=0.0, maxval=math.log(10.0))) / 3.0
    time_scale = jnp.exp(jax.random.uniform(key_time, (TT,), minval=math.log(0.3), maxval=math.log(3.0)))
    values = jnp.clip(jax.random.normal(key_noise, (TT, 3, P_SIZE)), -5.0, 5.0)
    return (values * time_scale[:, None, None] * space_scale[None, None, :]).astype(jnp.bfloat16)


def draw_block_starts(key, part):
    jitter = jax.random.randint(key, (NB,), 0, JIT + 1)
    return (jnp.arange(NB, dtype=jnp.int32) * HOP + jitter).astype(jnp.int32)


def set_ends(drawn, rng, low, top_value):
    dims = drawn.shape
    index_at = [jax.random.randint(jax.random.fold_in(rng, axis), (), 0, dims[axis]) for axis in range(len(dims))]
    drawn = drawn.at[tuple(index_at)].set(low)
    longest = dims.index(max(dims))
    index_at[longest] = (index_at[longest] + 1) % dims[longest]
    return drawn.at[tuple(index_at)].set(top_value)


def setup_inputs(seed: int = 0) -> dict:
    key_list = jax.random.split(jax.random.key(seed), 4)
    return {
        "snapshots": draw_snapshots(jax.random.fold_in(key_list[3], 71), 0),
        "block_starts": draw_block_starts(jax.random.fold_in(key_list[3], 71), 0),
        "freq_index": set_ends(jax.random.randint(key_list[2], (NF,), 0, NFFT // 2 + 1), jax.random.fold_in(key_list[2], 1), 0, (NFFT // 2 + 1) - 1).astype(jnp.int32),
    }


def dft_rows(freq_index):
    times_idx = jnp.arange(NFFT, dtype=jnp.int32)
    phase_int = freq_index[:, None].astype(jnp.int32) * times_idx[None, :] % NFFT
    angles = 2.0 * math.pi / NFFT * phase_int.astype(jnp.float32)
    window = 0.5 - 0.5 * jnp.cos(2.0 * math.pi / NFFT * times_idx.astype(jnp.float32))
    scaling = 1.0 / jnp.sqrt(jnp.sum(window * window))
    cosine = window[None, :] * jnp.cos(angles) * scaling
    sine_rows = -window[None, :] * jnp.sin(angles) * scaling
    return jnp.stack([cosine, sine_rows], 1).reshape(2 * NF, NFFT).astype(jnp.bfloat16)

def block_rows(block_starts):
    return block_starts[:, None].astype(jnp.int32) + jnp.arange(NFFT, dtype=jnp.int32)[None, :]

def matmul_batch(left, right):
    return jnp.einsum('fij,fjk->fik', left, right, precision=lax.Precision.HIGHEST)

def whiten(summed, points):
    gram_re = summed[:, 0]
    gram_im = summed[:, 1]
    top_rows = jnp.concatenate([gram_re, -gram_im], 2)
    low_rows = jnp.concatenate([gram_im, gram_re], 2)
    hermit = jnp.concatenate([top_rows, low_rows], 1)
    frob = jnp.sqrt(lax.optimization_barrier(jnp.sum(hermit * hermit, axis=(1, 2))) + 1e-06)
    identity = jnp.eye(2 * NB, dtype=jnp.float32)[None]
    iterate = hermit / frob[:, None, None]
    inverse = jnp.broadcast_to(identity, hermit.shape)
    for iteration in range(NSIT):
        factor = 1.5 * identity - 0.5 * matmul_batch(inverse, iterate)
        iterate = matmul_batch(iterate, factor)
        inverse = matmul_batch(factor, inverse)
    columns = inverse[:, :, :NB] * jnp.sqrt(6.0 * points / frob)[:, None, None]
    upper = columns[:, :NB]
    lower = columns[:, NB:]
    coefficients = jnp.stack([jnp.stack([upper, -lower], 1), jnp.stack([lower, upper], 1)], 1)
    energy = jnp.trace(gram_re, axis1=1, axis2=2) / (3.0 * NB * points)
    return (coefficients, energy)

def reference(snapshots, block_starts, freq_index):
    dft_table = dft_rows(freq_index).astype(jnp.float32)
    offsets = block_rows(block_starts)
    columns_all = snapshots.reshape(TT, 3 * P_SIZE)
    block_cols = 16 * P_DEV

    def spectra_block(start):
        piece = lax.dynamic_slice_in_dim(columns_all, start, block_cols, 1)
        windows = jnp.take(piece, offsets, axis=0).astype(jnp.float32)
        return jnp.einsum('rt,btn->brn', dft_table, windows, precision=lax.Precision.HIGHEST).astype(jnp.bfloat16)
    starts = jnp.arange(3 * P_SIZE // block_cols, dtype=jnp.int32) * block_cols
    pieces = lax.map(spectra_block, starts)
    spectra = jnp.transpose(pieces, (1, 2, 0, 3)).reshape(NB, NF, 2, 3 * P_SIZE)
    by_freq = jnp.moveaxis(spectra, 1, 0)

    def gram_one(spec_f):
        real_part = spec_f[:, 0].astype(jnp.float32)
        imag_part = spec_f[:, 1].astype(jnp.float32)
        gram_re = jnp.dot(real_part, real_part.T, precision=lax.Precision.HIGHEST) + jnp.dot(imag_part, imag_part.T, precision=lax.Precision.HIGHEST)
        cross_terms = jnp.dot(real_part, imag_part.T, precision=lax.Precision.HIGHEST)
        return jnp.stack([gram_re, cross_terms - cross_terms.T])
    summed = lax.map(gram_one, by_freq)
    coefficients, energy = whiten(summed, float(P_SIZE))
    coef_bf = coefficients.astype(jnp.bfloat16)

    def modes_one(pair):
        coef_f, spec_f = pair
        return jnp.einsum('orbj,brn->jon', coef_f.astype(jnp.float32), spec_f.astype(jnp.float32), precision=lax.Precision.HIGHEST).astype(jnp.bfloat16)
    modes = lax.map(modes_one, (coef_bf, by_freq))
    return (modes.reshape(NF, NB, 2, 3, P_SIZE), energy)
```

```python
import functools
import math

import jax
import jax.numpy as jnp
from jax import lax
from jax.experimental import pallas as pl
from jax.experimental.pallas import tpu as pltpu
from jax.sharding import PartitionSpec as P

NB = 32
NFFT = 256
NF = 16
NSIT = 6
SLABS = 8
PEERS = 8
ROWS = 68
OWN = 4
WB = 8
LANES = 128
POINTS = 32768.0
MESH = pl.DeviceIdType.MESH


def dft_rows(freq_index):
    times_idx = jnp.arange(NFFT, dtype=jnp.int32)
    phase_int = freq_index[:, None] * times_idx[None, :] % NFFT
    angles = 2.0 * math.pi / NFFT * phase_int.astype(jnp.float32)
    window = 0.5 - 0.5 * jnp.cos(2.0 * math.pi / NFFT * times_idx.astype(jnp.float32))
    scaling = 1.0 / jnp.sqrt(jnp.sum(window * window))
    cosine = window[None, :] * jnp.cos(angles) * scaling
    sine_rows = -window[None, :] * jnp.sin(angles) * scaling
    return jnp.stack([cosine, sine_rows], 1).reshape(2 * NF, NFFT).astype(jnp.bfloat16)


def one_hot_rows(rows, cols, source):
    i = lax.broadcasted_iota(jnp.int32, (rows, cols), 0)
    j = lax.broadcasted_iota(jnp.int32, (rows, cols), 1)
    return jnp.where(source(i) == j, 1.0, 0.0).astype(jnp.bfloat16)


def dot_nn(a, b, precision=None):
    return lax.dot_general(
        a, b, (((1,), (0,)), ((), ())), precision=precision, preferred_element_type=jnp.float32
    )


def dot_nt(a, b, precision=None):
    return lax.dot_general(
        a, b, (((1,), (1,)), ((), ())), precision=precision, preferred_element_type=jnp.float32
    )


def step_slab(step):
    return lax.rem(step, 2) * 4 + lax.rem(step // 2, 2) * 2 + step // 4


def kernel(
    xt,
    table,
    starts,
    out,
    energy_out,
    weights,
    rbuf,
    own,
    hsend,
    hrecv,
    zsend,
    spec,
    sxy,
    gsend,
    grecv,
    bsend,
    brecv,
    csend,
    crecv,
    ysend_sem,
    yrecv_sem,
    hsend_sem,
    hrecv_sem,
    zsend_sem,
    zrecv_sem,
    gsend_sem,
    grecv_sem,
    bsend_sem,
    brecv_sem,
    csend_sem,
    crecv_sem,
):
    tm = lax.axis_index("tm")
    fx = lax.axis_index("freq")
    z = tm // PEERS
    me = lax.rem(tm, PEERS)
    y = me // 2
    core = lax.rem(me, 2)

    def slab_peer(p):
        return {"tm": z * PEERS + p, "freq": fx}

    def column_peer(zz):
        return {"tm": zz * PEERS + me, "freq": fx}

    def plane_peer(k):
        return {"tm": z * PEERS + lax.rem(k, 4) * 2 + core, "freq": k // 4}

    def line_peer(k):
        return {"tm": (k // 2) * PEERS + y * 2 + lax.rem(k, 2), "freq": fx}

    plane_me = fx * 4 + y
    line_me = z * 2 + core

    hrecv[...] = jnp.zeros_like(hrecv)

    barrier = pltpu.get_barrier_semaphore()

    def greet(device):
        pl.semaphore_signal(barrier, inc=1, device_id=device, device_id_type=MESH)

    @pl.loop(1, PEERS)
    def _(d):
        greet(slab_peer(lax.rem(me + d, PEERS)))

    @pl.loop(1, 16)
    def _(d):
        greet(plane_peer(lax.rem(plane_me + d, 16)))
        greet(line_peer(lax.rem(line_me + d, 16)))

    pl.semaphore_wait(barrier, 37)

    def y_copy(zz, p):
        cols = pl.ds(pl.multiple_of((zz * PEERS + p) * LANES, LANES), LANES)
        return pltpu.make_async_remote_copy(
            src_ref=xt.at[:, :, cols],
            dst_ref=rbuf.at[zz, me],
            send_sem=ysend_sem.at[zz, p],
            recv_sem=yrecv_sem.at[zz, me],
            device_id=slab_peer(p),
            device_id_type=MESH,
        )

    def y_local(zz):
        cols = pl.ds(pl.multiple_of((zz * PEERS + me) * LANES, LANES), LANES)
        return pltpu.make_async_copy(xt.at[:, :, cols], rbuf.at[zz, me], yrecv_sem.at[zz, me])

    @pl.loop(0, SLABS)
    def _(s):
        zz = step_slab(s)
        y_local(zz).start()

        @pl.loop(1, PEERS)
        def _(d):
            y_copy(zz, lax.rem(me + d, PEERS)).start()

    tau = lax.broadcasted_iota(jnp.int32, (NFFT, ROWS), 0)
    tt = lax.broadcasted_iota(jnp.int32, (NFFT, ROWS), 1)
    for i in range(WB):
        b = z * OWN - 2 + i
        first = starts[jnp.clip(b, 0, NB - 1)]
        for src in range(PEERS):
            origin = z * (PEERS * ROWS) + src * ROWS
            pick = jnp.where(tau + first == tt + origin, 1.0, 0.0).astype(jnp.bfloat16)
            weights[src, pl.ds(i * 32, 32), :] = dot_nn(table[...], pick).astype(jnp.bfloat16)

    order = one_hot_rows(128, 128, lambda i: lax.rem(i // 2, 4) * 32 + (i // 8) * 2 + lax.rem(i, 2))

    def h_copy(zz, slot, target):
        return pltpu.make_async_remote_copy(
            src_ref=hsend.at[zz, slot],
            dst_ref=hrecv.at[zz, slot],
            send_sem=hsend_sem.at[zz, slot],
            recv_sem=hrecv_sem.at[zz, slot],
            device_id=column_peer(target),
            device_id_type=MESH,
        )

    def helpers(zz, act_send, act_recv):
        up = jnp.minimum(z + 1, SLABS - 1)
        down = jnp.maximum(z - 1, 0)
        for slot, target, sends, takes in (
            (0, up, z <= 6, z >= 1),
            (1, up, (z >= 4) & (z <= 6), z >= 5),
            (2, down, z == 1, z == 0),
            (3, down, (z >= 1) & (z <= 5), z <= 4),
        ):
            if act_send is not None:

                @pl.when(sends)
                def _():
                    act_send(h_copy(zz, slot, target))

            if act_recv is not None:

                @pl.when(takes)
                def _():
                    act_recv(h_copy(zz, slot, target))

    def z_copy(zz, target):
        return pltpu.make_async_remote_copy(
            src_ref=zsend.at[zz],
            dst_ref=spec.at[z],
            send_sem=zsend_sem.at[zz],
            recv_sem=zrecv_sem.at[z],
            device_id=column_peer(target),
            device_id_type=MESH,
        )

    def partial(s):
        zz = step_slab(s)
        y_local(zz).wait()

        @pl.loop(1, PEERS)
        def _(d):
            p = lax.rem(me + d, PEERS)
            pltpu.make_async_remote_copy(
                src_ref=rbuf.at[zz, p],
                dst_ref=rbuf.at[zz, p],
                send_sem=ysend_sem.at[zz, p],
                recv_sem=yrecv_sem.at[zz, p],
                device_id=slab_peer(p),
                device_id_type=MESH,
            ).wait_recv()

        for c in range(3):
            acc = dot_nn(weights[0], rbuf[zz, 0, c])
            for src in range(1, PEERS):
                acc = acc + dot_nn(weights[src], rbuf[zz, src, c])
            cols = pl.ds(c * LANES, LANES)
            acc = acc.reshape(WB, 32, LANES)
            hsend[zz, 2:4, :, cols] = acc[0:2]
            own[lax.rem(s, 2), :, :, cols] = acc[2:6]
            hsend[zz, 0:2, :, cols] = acc[6:8]
        helpers(zz, lambda copy: copy.start(), None)

    def finish(s):
        zz = step_slab(s)
        helpers(zz, None, lambda copy: copy.wait_recv())
        total = (own[lax.rem(s, 2)] + hrecv[zz]).astype(jnp.bfloat16).reshape(OWN * 32, 3 * LANES)
        rows = dot_nn(order, total).astype(jnp.bfloat16)
        for c in range(3):
            zsend[zz, c] = rows[:, c * LANES : (c + 1) * LANES]

        @pl.when(zz == z)
        def _():
            pltpu.make_async_copy(zsend.at[zz], spec.at[z], zrecv_sem.at[z]).start()

        @pl.when(zz != z)
        def _():
            z_copy(zz, zz).start()

    partial(0)

    @pl.loop(1, SLABS)
    def _(s):
        partial(s)
        finish(s - 1)

    finish(SLABS - 1)

    pltpu.make_async_copy(zsend.at[z], spec.at[z], zrecv_sem.at[z]).wait()

    @pl.loop(1, SLABS)
    def _(d):
        zz = lax.rem(z + d, SLABS)
        pltpu.make_async_remote_copy(
            src_ref=spec.at[zz],
            dst_ref=spec.at[zz],
            send_sem=zsend_sem.at[zz],
            recv_sem=zrecv_sem.at[zz],
            device_id=column_peer(zz),
            device_id_type=MESH,
        ).wait_recv()

    arrange = one_hot_rows(
        128,
        128,
        lambda i: (lax.rem(i, 32) // 4) * 16
        + (i // 64) * 8
        + lax.rem(i, 4) * 2
        + lax.rem(i // 32, 2),
    )
    for pair in range(NF // 2):
        grams = [None, None]
        for c in range(3):
            stacked = spec[:, c, pl.ds(pair * 16, 16), :].reshape(128, LANES)
            placed = dot_nn(arrange, stacked).astype(jnp.bfloat16)
            sxy[pair, c] = placed
            for h in range(2):
                xr = placed[h * 64 : h * 64 + 32]
                yr = placed[h * 64 + 32 : h * 64 + 64]
                left = jnp.concatenate([xr, -yr], 0)
                right = jnp.concatenate([yr, xr], 0)
                term = dot_nt(left, xr) + dot_nt(right, yr)
                grams[h] = term if c == 0 else grams[h] + term
        for h in range(2):
            g = grams[h]
            gsend[pair * 2 + h] = jnp.concatenate([g[16 * k : 16 * k + 16] for k in range(4)], 1)

    def g_copy(k):
        return pltpu.make_async_remote_copy(
            src_ref=gsend.at[k],
            dst_ref=grecv.at[plane_me],
            send_sem=gsend_sem.at[k],
            recv_sem=grecv_sem.at[plane_me],
            device_id=plane_peer(k),
            device_id_type=MESH,
        )

    @pl.loop(1, 16)
    def _(d):
        g_copy(lax.rem(plane_me + d, 16)).start()

    grecv[plane_me] = gsend[plane_me]

    @pl.loop(1, 16)
    def _(d):
        k = lax.rem(plane_me + d, 16)
        pltpu.make_async_remote_copy(
            src_ref=grecv.at[k],
            dst_ref=grecv.at[k],
            send_sem=gsend_sem.at[k],
            recv_sem=grecv_sem.at[k],
            device_id=plane_peer(k),
            device_id_type=MESH,
        ).wait_recv()

    bsend[...] = jnp.sum(grecv[...], axis=0)

    @pl.loop(1, 16)
    def _(d):
        k = lax.rem(line_me + d, 16)
        pltpu.make_async_remote_copy(
            src_ref=bsend,
            dst_ref=brecv.at[line_me],
            send_sem=bsend_sem.at[k],
            recv_sem=brecv_sem.at[line_me],
            device_id=line_peer(k),
            device_id_type=MESH,
        ).start()

    brecv[line_me] = bsend[...]

    @pl.loop(1, 16)
    def _(d):
        k = lax.rem(line_me + d, 16)
        pltpu.make_async_remote_copy(
            src_ref=brecv.at[k],
            dst_ref=brecv.at[k],
            send_sem=bsend_sem.at[k],
            recv_sem=brecv_sem.at[k],
            device_id=line_peer(k),
            device_id_type=MESH,
        ).wait_recv()

    packed = jnp.sum(brecv[...], axis=0)
    gram = jnp.concatenate([packed[:, 32 * k : 32 * k + 32] for k in range(4)], 0)
    gram_re, gram_im = gram[:NB], gram[NB:]
    hermit = jnp.concatenate(
        [jnp.concatenate([gram_re, -gram_im], 1), jnp.concatenate([gram_im, gram_re], 1)], 0
    )
    eye = jnp.where(
        lax.broadcasted_iota(jnp.int32, (64, 64), 0) == lax.broadcasted_iota(jnp.int32, (64, 64), 1),
        1.0,
        0.0,
    )
    square = jnp.sum(jnp.sum(hermit * hermit, axis=1, keepdims=True), axis=0, keepdims=True)
    frob = jnp.sqrt(square + 1e-06)
    trace = jnp.sum(jnp.sum(gram_re * eye[:NB, :NB], axis=1, keepdims=True), axis=0, keepdims=True)
    energy = jnp.broadcast_to(trace / (3.0 * NB * POINTS), (16, LANES))
    iterate = hermit / frob
    inverse = eye
    high = lax.Precision.HIGHEST
    for iteration in range(NSIT):
        if iteration == 0:
            factor = 1.5 * eye - 0.5 * iterate
            inverse = factor
        else:
            factor = 1.5 * eye - 0.5 * dot_nn(inverse, iterate, high)
            inverse = dot_nn(factor, inverse, high)
        if iteration < NSIT - 1:
            iterate = dot_nn(iterate, factor, high)
    columns = inverse[:, :NB] * jnp.sqrt(6.0 * POINTS / frob)
    upper, lower = columns[:NB], columns[NB:]
    coef = jnp.concatenate(
        [jnp.concatenate([upper, lower], 1), jnp.concatenate([-lower, upper], 1)], 0
    ).astype(jnp.bfloat16)
    high_part = energy.astype(jnp.bfloat16)
    rest = energy - high_part.astype(jnp.float32)
    mid_part = rest.astype(jnp.bfloat16)
    low_part = (rest - mid_part.astype(jnp.float32)).astype(jnp.bfloat16)
    csend[0:32, :] = jnp.concatenate([coef[:NB], coef[NB:]], 1)
    csend[32:48, :] = high_part
    csend[48:64, :] = mid_part
    csend[64:80, :] = low_part

    @pl.loop(1, 16)
    def _(d):
        k = lax.rem(plane_me + d, 16)
        pltpu.make_async_remote_copy(
            src_ref=csend,
            dst_ref=crecv.at[plane_me],
            send_sem=csend_sem.at[k],
            recv_sem=crecv_sem.at[plane_me],
            device_id=plane_peer(k),
            device_id_type=MESH,
        ).start()

    crecv[plane_me] = csend[...]

    @pl.loop(1, 16)
    def _(d):
        k = lax.rem(plane_me + d, 16)
        pltpu.make_async_remote_copy(
            src_ref=crecv.at[k],
            dst_ref=crecv.at[k],
            send_sem=csend_sem.at[k],
            recv_sem=crecv_sem.at[k],
            device_id=plane_peer(k),
            device_id_type=MESH,
        ).wait_recv()

    pick_row = one_hot_rows(192, 64, lambda i: lax.rem(i, 2) * 32 + i // 6)
    row_c = lax.rem(lax.broadcasted_iota(jnp.int32, (192, 192), 0) // 2, 3)
    col_c = lax.broadcasted_iota(jnp.int32, (192, 192), 1) // 64
    same_c = row_c == col_c
    for f in range(NF):
        message = crecv[f]
        coef_f = jnp.concatenate([message[0:32, 0:64], message[0:32, 64:128]], 0)
        wide = lax.dot_general(
            pick_row, coef_f, (((1,), (1,)), ((), ())), preferred_element_type=jnp.float32
        )
        wide = jnp.where(same_c, jnp.concatenate([wide, wide, wide], 1), 0.0).astype(jnp.bfloat16)
        stacked = jnp.concatenate(
            [sxy[f // 2, c, pl.ds((f % 2) * 64, 64), :] for c in range(3)], 0
        )
        out[pl.ds(f * 192, 192), :] = dot_nn(wide, stacked).astype(jnp.bfloat16)
        energy_out[pl.ds(f, 1), :] = (
            message[32:48].astype(jnp.float32)
            + message[48:64].astype(jnp.float32)
            + message[64:80].astype(jnp.float32)
        )[0:1]

    @pl.loop(0, SLABS)
    def _(s):
        @pl.loop(1, PEERS)
        def _(d):
            y_copy(s, lax.rem(me + d, PEERS)).wait_send()

        helpers(s, lambda copy: copy.wait_send(), None)

        @pl.when(s != z)
        def _():
            z_copy(s, s).wait_send()

    @pl.loop(1, 16)
    def _(d):
        k = lax.rem(plane_me + d, 16)
        g_copy(k).wait_send()
        pltpu.make_async_remote_copy(
            src_ref=csend,
            dst_ref=crecv.at[plane_me],
            send_sem=csend_sem.at[k],
            recv_sem=crecv_sem.at[plane_me],
            device_id=plane_peer(k),
            device_id_type=MESH,
        ).wait_send()
        q = lax.rem(line_me + d, 16)
        pltpu.make_async_remote_copy(
            src_ref=bsend,
            dst_ref=brecv.at[line_me],
            send_sem=bsend_sem.at[q],
            recv_sem=brecv_sem.at[line_me],
            device_id=line_peer(q),
            device_id_type=MESH,
        ).wait_send()


def local(snapshots, block_starts, freq_index):
    xt = jnp.transpose(snapshots, (1, 0, 2))
    table = dft_rows(freq_index)
    dma = pltpu.SemaphoreType.DMA
    vmem = pltpu.VMEM
    bf, f32 = jnp.bfloat16, jnp.float32
    modes, energy = pl.pallas_call(
        kernel,
        out_shape=(
            jax.ShapeDtypeStruct((NF * 192, LANES), bf),
            jax.ShapeDtypeStruct((NF, LANES), f32),
        ),
        in_specs=[
            pl.BlockSpec(memory_space=pl.ANY),
            pl.BlockSpec(memory_space=pltpu.VMEM),
            pl.BlockSpec(memory_space=pltpu.SMEM),
        ],
        out_specs=(
            pl.BlockSpec(memory_space=pltpu.VMEM),
            pl.BlockSpec(memory_space=pltpu.VMEM),
        ),
        scratch_shapes=[
            vmem((PEERS, WB * 32, ROWS), bf),
            vmem((SLABS, PEERS, 3, ROWS, LANES), bf),
            vmem((2, OWN, 32, 3 * LANES), f32),
            vmem((SLABS, 4, 32, 3 * LANES), f32),
            vmem((SLABS, 4, 32, 3 * LANES), f32),
            vmem((SLABS, 3, 128, LANES), bf),
            vmem((SLABS, 3, 128, LANES), bf),
            vmem((NF // 2, 3, 128, LANES), bf),
            vmem((NF, 16, LANES), f32),
            vmem((NF, 16, LANES), f32),
            vmem((16, LANES), f32),
            vmem((16, 16, LANES), f32),
            vmem((80, LANES), bf),
            vmem((16, 80, LANES), bf),
            dma((SLABS, PEERS)),
            dma((SLABS, PEERS)),
            dma((SLABS, 4)),
            dma((SLABS, 4)),
            dma((SLABS,)),
            dma((SLABS,)),
            dma((16,)),
            dma((16,)),
            dma((16,)),
            dma((16,)),
            dma((16,)),
            dma((16,)),
        ],
        compiler_params=pltpu.CompilerParams(collective_id=0, has_side_effects=True),
        name="modes",
    )(xt, table, block_starts)
    modes = modes.reshape(NF, NB, 3, 2, LANES)
    return (jnp.transpose(modes, (0, 1, 3, 2, 4)), energy[:, 0])


def solution(mesh):
    return jax.shard_map(
        local,
        mesh=mesh,
        in_specs=(P("tm", None, "freq"), P(), P()),
        out_specs=(P(None, None, None, None, ("freq", "tm")), P()),
        check_vma=False,
    )
```

```python
import functools
import math

import jax
import jax.numpy as jnp
from jax import lax
from jax.experimental import pallas as pl
from jax.experimental.pallas import tpu as pltpu
from jax.sharding import PartitionSpec as P

NB = 32
NFFT = 256
NF = 16
NSIT = 6
SLABS = 8
PEERS = 8
ROWS = 68
OWN = 4
WB = 8
UNITS = 3 * SLABS
AHEAD = 6
LAG = 3
STEP = 16
LANES = 128
POINTS = 32768.0
MESH = pl.DeviceIdType.MESH


def dft_rows(freq):
    row = lax.broadcasted_iota(jnp.int32, (2 * NF, NFFT), 0)
    time = lax.broadcasted_iota(jnp.int32, (2 * NF, NFFT), 1)
    bins = jnp.zeros((2 * NF, NFFT), jnp.int32)
    for f in range(NF):
        bins = jnp.where(row // 2 == f, freq[f], bins)
    angles = 2.0 * math.pi / NFFT * lax.rem(bins * time, NFFT).astype(jnp.float32)
    window = 0.5 - 0.5 * jnp.cos(2.0 * math.pi / NFFT * time[0:8].astype(jnp.float32))
    scaling = 1.0 / jnp.sqrt(jnp.sum((window * window)[0:1], axis=1, keepdims=True))
    window = jnp.concatenate([window] * (2 * NF // 8), 0)
    wave = jnp.where(lax.rem(row, 2) == 0, window * jnp.cos(angles), -window * jnp.sin(angles))
    return (wave * scaling).astype(jnp.bfloat16)


def one_hot_rows(rows, cols, source):
    i = lax.broadcasted_iota(jnp.int32, (rows, cols), 0)
    j = lax.broadcasted_iota(jnp.int32, (rows, cols), 1)
    return jnp.where(source(i) == j, 1.0, 0.0).astype(jnp.bfloat16)


def dot_nn(a, b, precision=None):
    return lax.dot_general(
        a, b, (((1,), (0,)), ((), ())), precision=precision, preferred_element_type=jnp.float32
    )


def dot_nt(a, b, precision=None):
    return lax.dot_general(
        a, b, (((1,), (1,)), ((), ())), precision=precision, preferred_element_type=jnp.float32
    )


def step_slab(step):
    return lax.rem(step, 2) * 4 + lax.rem(step // 2, 2) * 2 + step // 4


def kernel(
    xt,
    starts_hbm,
    freq_hbm,
    sxy,
    coef_out,
    starts,
    freq,
    weights,
    rbuf,
    own,
    hsend,
    hrecv,
    zsend,
    spec,
    gacc,
    gsend,
    grecv,
    bsend,
    brecv,
    csend,
    crecv,
    ysend_sem,
    yrecv_sem,
    hsend_sem,
    hrecv_sem,
    zsend_sem,
    zrecv_sem,
    gsend_sem,
    grecv_sem,
    bsend_sem,
    brecv_sem,
    csend_sem,
    crecv_sem,
    small_sem,
):
    tm = lax.axis_index("tm")
    fx = lax.axis_index("freq")
    z = tm // PEERS
    me = lax.rem(tm, PEERS)
    y = me // 2
    core = lax.rem(me, 2)

    def slab_peer(p):
        return {"tm": z * PEERS + p, "freq": fx}

    def column_peer(zz):
        return {"tm": zz * PEERS + me, "freq": fx}

    def plane_peer(k):
        return {"tm": z * PEERS + lax.rem(k, 4) * 2 + core, "freq": k // 4}

    def line_peer(k):
        return {"tm": (k // 2) * PEERS + y * 2 + lax.rem(k, 2), "freq": fx}

    plane_me = fx * 4 + y
    line_me = z * 2 + core

    starts_copy = pltpu.make_async_copy(starts_hbm, starts, small_sem.at[0])
    freq_copy = pltpu.make_async_copy(freq_hbm, freq, small_sem.at[1])
    starts_copy.start()
    freq_copy.start()

    barrier = pltpu.get_barrier_semaphore()

    def greet(device):
        pl.semaphore_signal(barrier, inc=1, device_id=device, device_id_type=MESH)

    @pl.loop(1, PEERS)
    def _(d):
        greet(slab_peer(lax.rem(me + d, PEERS)))

    @pl.loop(1, 16)
    def _(d):
        greet(plane_peer(lax.rem(plane_me + d, 16)))
        greet(line_peer(lax.rem(line_me + d, 16)))

    starts_copy.wait()
    freq_copy.wait()
    table = dft_rows(freq)
    pl.semaphore_wait(barrier, 37)

    def y_copy(c, zz, p):
        cols = pl.ds(pl.multiple_of((zz * PEERS + p) * LANES, LANES), LANES)
        return pltpu.make_async_remote_copy(
            src_ref=xt.at[c, :, cols],
            dst_ref=rbuf.at[c, zz, me],
            send_sem=ysend_sem.at[c, zz, p],
            recv_sem=yrecv_sem.at[c, zz, me],
            device_id=slab_peer(p),
            device_id_type=MESH,
        )

    def y_arrival(c, zz, p):
        return pltpu.make_async_remote_copy(
            src_ref=rbuf.at[c, zz, p],
            dst_ref=rbuf.at[c, zz, p],
            send_sem=ysend_sem.at[c, zz, p],
            recv_sem=yrecv_sem.at[c, zz, p],
            device_id=slab_peer(p),
            device_id_type=MESH,
        )

    def y_local(c, zz):
        cols = pl.ds(pl.multiple_of((zz * PEERS + me) * LANES, LANES), LANES)
        return pltpu.make_async_copy(
            xt.at[c, :, cols], rbuf.at[c, zz, me], yrecv_sem.at[c, zz, me]
        )

    def y_start(u):
        c, zz = u // SLABS, step_slab(lax.rem(u, SLABS))

        @pl.loop(1, PEERS)
        def _(d):
            y_copy(c, zz, lax.rem(me + d, PEERS)).start()

        y_local(c, zz).start()

    @pl.loop(0, AHEAD)
    def _(u):
        y_start(u)

    tau = lax.broadcasted_iota(jnp.int32, (NFFT, ROWS), 0)
    tt = lax.broadcasted_iota(jnp.int32, (NFFT, ROWS), 1)
    lag = tau - tt
    for i in range(WB):
        b = z * OWN - 2 + i
        first = starts[jnp.clip(b, 0, NB - 1)]
        for src in range(PEERS):
            origin = z * (PEERS * ROWS) + src * ROWS
            pick = jnp.where(lag == origin - first, 1.0, 0.0).astype(jnp.bfloat16)
            weights[src, pl.ds(i * 32, 32), :] = dot_nn(table, pick).astype(jnp.bfloat16)

    order = one_hot_rows(128, 128, lambda i: lax.rem(i // 2, 4) * 32 + (i // 8) * 2 + lax.rem(i, 2))
    arrange = one_hot_rows(
        128,
        128,
        lambda i: (lax.rem(i, 32) // 4) * 16
        + (i // 64) * 8
        + lax.rem(i, 4) * 2
        + lax.rem(i // 32, 2),
    )

    def h_copy(c, zz, slot, target):
        return pltpu.make_async_remote_copy(
            src_ref=hsend.at[c, zz, slot],
            dst_ref=hrecv.at[c, zz, slot],
            send_sem=hsend_sem.at[c, zz, slot],
            recv_sem=hrecv_sem.at[c, zz, slot],
            device_id=column_peer(target),
            device_id_type=MESH,
        )

    def helpers(c, zz, act_send=None, act_take=None):
        up = jnp.minimum(z + 1, SLABS - 1)
        down = jnp.maximum(z - 1, 0)
        for slot, target, sends, takes in (
            (0, up, z <= 6, z >= 1),
            (1, up, (z >= 4) & (z <= 6), z >= 5),
            (2, down, z == 1, z == 0),
            (3, down, (z >= 1) & (z <= 5), z <= 4),
        ):
            if act_send is not None:

                @pl.when(sends)
                def _():
                    act_send(h_copy(c, zz, slot, target))

            if act_take is not None:

                @pl.when(takes)
                def _():
                    act_take(h_copy(c, zz, slot, target), slot)

    def z_copy(c, zz):
        return pltpu.make_async_remote_copy(
            src_ref=zsend.at[c, zz],
            dst_ref=spec.at[c, z],
            send_sem=zsend_sem.at[c, zz],
            recv_sem=zrecv_sem.at[c, z],
            device_id=column_peer(zz),
            device_id_type=MESH,
        )

    def z_arrival(c, zz):
        return pltpu.make_async_remote_copy(
            src_ref=spec.at[c, zz],
            dst_ref=spec.at[c, zz],
            send_sem=zsend_sem.at[c, zz],
            recv_sem=zrecv_sem.at[c, zz],
            device_id=column_peer(zz),
            device_id_type=MESH,
        )

    def partial(u):
        c, zz, slot = u // SLABS, step_slab(lax.rem(u, SLABS)), lax.rem(u, LAG + 1)
        y_local(c, zz).wait()

        @pl.loop(1, PEERS)
        def _(d):
            y_arrival(c, zz, lax.rem(me + d, PEERS)).wait_recv()

        acc = dot_nn(weights[0], rbuf[c, zz, 0])
        for src in range(1, PEERS):
            acc = acc + dot_nn(weights[src], rbuf[c, zz, src])
        acc = acc.reshape(WB, 32, LANES)
        hsend[c, zz, 2:4] = acc[0:2]
        hsend[c, zz, 0:2] = acc[6:8]
        own[slot] = acc[2:6]
        helpers(c, zz, act_send=lambda copy: copy.start())

    def finish(u):
        c, zz, slot = u // SLABS, step_slab(lax.rem(u, SLABS)), lax.rem(u, LAG + 1)

        def take(copy, i):
            copy.wait_recv()
            own[slot, i] = own[slot, i] + hrecv[c, zz, i]

        helpers(c, zz, act_take=take)
        total = own[slot].astype(jnp.bfloat16).reshape(OWN * 32, LANES)
        rows = dot_nn(order, total).astype(jnp.bfloat16)

        @pl.when(zz == z)
        def _():
            spec[c, z] = rows

        @pl.when(zz != z)
        def _():
            zsend[c, zz] = rows
            z_copy(c, zz).start()

    def pipeline(first, last):
        @pl.loop(first, last)
        def _(u):
            partial(u)

            @pl.when(u + AHEAD < UNITS)
            def _():
                y_start(u + AHEAD)

            @pl.when(u >= LAG)
            def _():
                finish(u - LAG)

    def gather(c):
        @pl.loop(1, SLABS)
        def _(d):
            z_arrival(c, lax.rem(z + d, SLABS)).wait_recv()

        for pair in range(NF // 2):
            stacked = spec[c, :, pl.ds(pair * 16, 16), :].reshape(128, LANES)
            placed = dot_nn(arrange, stacked).astype(jnp.bfloat16)
            sxy[2 * pair, c] = placed[0:64]
            sxy[2 * pair + 1, c] = placed[64:128]
            products = dot_nt(placed, placed)
            if c > 0:
                products = products + gacc[pair]
            if c < 2:
                gacc[pair] = products
            else:
                for h in range(2):
                    k = h * 64
                    xx = products[k : k + 32, k : k + 32]
                    yy = products[k + 32 : k + 64, k + 32 : k + 64]
                    xy = products[k : k + 32, k + 32 : k + 64]
                    yx = products[k + 32 : k + 64, k : k + 32]
                    both = jnp.where(on_or_above, xx + yy, xy - yx)
                    gsend[2 * pair + h] = jnp.concatenate(
                        [both[8 * q : 8 * q + 8] for q in range(4)], 1
                    )

    row32 = lax.broadcasted_iota(jnp.int32, (NB, NB), 0)
    col32 = lax.broadcasted_iota(jnp.int32, (NB, NB), 1)
    on_or_above = col32 >= row32

    pipeline(0, 15)
    gather(0)
    pipeline(15, 23)
    gather(1)
    pipeline(23, UNITS)

    @pl.loop(UNITS - LAG, UNITS)
    def _(u):
        finish(u)

    gather(2)

    def g_copy(k):
        return pltpu.make_async_remote_copy(
            src_ref=gsend.at[k],
            dst_ref=grecv.at[plane_me],
            send_sem=gsend_sem.at[k],
            recv_sem=grecv_sem.at[plane_me],
            device_id=plane_peer(k),
            device_id_type=MESH,
        )

    def g_arrival(k):
        return pltpu.make_async_remote_copy(
            src_ref=grecv.at[k],
            dst_ref=grecv.at[k],
            send_sem=gsend_sem.at[k],
            recv_sem=grecv_sem.at[k],
            device_id=plane_peer(k),
            device_id_type=MESH,
        )

    def b_copy(k):
        return pltpu.make_async_remote_copy(
            src_ref=bsend,
            dst_ref=brecv.at[line_me],
            send_sem=bsend_sem.at[k],
            recv_sem=brecv_sem.at[line_me],
            device_id=line_peer(k),
            device_id_type=MESH,
        )

    def b_arrival(k):
        return pltpu.make_async_remote_copy(
            src_ref=brecv.at[k],
            dst_ref=brecv.at[k],
            send_sem=bsend_sem.at[k],
            recv_sem=brecv_sem.at[k],
            device_id=line_peer(k),
            device_id_type=MESH,
        )

    def c_copy(k):
        return pltpu.make_async_remote_copy(
            src_ref=csend,
            dst_ref=crecv.at[plane_me],
            send_sem=csend_sem.at[k],
            recv_sem=crecv_sem.at[plane_me],
            device_id=plane_peer(k),
            device_id_type=MESH,
        )

    def c_arrival(k):
        return pltpu.make_async_remote_copy(
            src_ref=crecv.at[k],
            dst_ref=crecv.at[k],
            send_sem=csend_sem.at[k],
            recv_sem=crecv_sem.at[k],
            device_id=plane_peer(k),
            device_id_type=MESH,
        )

    def others(mine, act):
        @pl.loop(1, 16)
        def _(d):
            act(lax.rem(mine + d, 16))

    others(plane_me, lambda k: g_copy(k).start())
    grecv[plane_me] = gsend[plane_me]

    @pl.loop(0, UNITS)
    def _(u):
        c, zz = u // SLABS, lax.rem(u, SLABS)

        @pl.loop(1, PEERS)
        def _(d):
            y_copy(c, zz, lax.rem(me + d, PEERS)).wait_send()

    others(plane_me, lambda k: g_arrival(k).wait_recv())
    bsend[...] = jnp.sum(grecv[...], axis=0)

    others(line_me, lambda k: b_copy(k).start())
    brecv[line_me] = bsend[...]

    @pl.loop(0, UNITS)
    def _(u):
        c, zz = u // SLABS, lax.rem(u, SLABS)
        helpers(c, zz, act_send=lambda copy: copy.wait_send())

        @pl.when(zz != z)
        def _():
            z_copy(c, zz).wait_send()

    others(plane_me, lambda k: g_copy(k).wait_send())
    others(line_me, lambda k: b_arrival(k).wait_recv())

    packed = jnp.sum(brecv[...], axis=0)
    both = jnp.concatenate([packed[:, 32 * k : 32 * k + 32] for k in range(4)], 0)
    flipped = both.T
    gram_re = jnp.where(on_or_above, both, flipped)
    gram_im = jnp.where(col32 < row32, both, jnp.where(col32 == row32, 0.0, -flipped))
    hermit = jnp.concatenate(
        [jnp.concatenate([gram_re, -gram_im], 1), jnp.concatenate([gram_im, gram_re], 1)], 0
    )
    row64 = lax.broadcasted_iota(jnp.int32, (64, 64), 0)
    eye = jnp.where(row64 == lax.broadcasted_iota(jnp.int32, (64, 64), 1), 1.0, 0.0)
    square = jnp.sum(jnp.sum(hermit * hermit, axis=1, keepdims=True), axis=0, keepdims=True)
    frob = jnp.sqrt(square + 1e-06)
    trace = jnp.sum(
        jnp.sum(jnp.where(col32 == row32, both, 0.0), axis=1, keepdims=True), axis=0, keepdims=True
    )
    iterate = hermit / frob
    high = lax.Precision.HIGHEST
    factor = 1.5 * eye - 0.5 * iterate
    inverse = factor
    iterate = dot_nn(iterate, factor, high)
    for iteration in range(1, NSIT):
        factor = 1.5 * eye - 0.5 * dot_nn(inverse, iterate, high)
        inverse = dot_nn(factor, inverse, high)
        if iteration < NSIT - 1:
            iterate = dot_nn(iterate, factor, high)
    columns = inverse[:, :NB] * jnp.sqrt(6.0 * POINTS / frob)
    energy = jnp.broadcast_to(trace / (3.0 * NB * POINTS), (16, LANES))
    high_part = energy.astype(jnp.bfloat16).astype(jnp.float32)
    mid_part = (energy - high_part).astype(jnp.bfloat16).astype(jnp.float32)
    low_part = energy - high_part - mid_part
    row16 = lax.broadcasted_iota(jnp.int32, (16, LANES), 0)
    parts = jnp.where(
        row16 == 0, high_part, jnp.where(row16 == 1, mid_part, jnp.where(row16 == 2, low_part, 0.0))
    )
    csend[0:16, :] = jnp.concatenate(
        [columns[16 * q : 16 * q + 16] for q in range(4)], 1
    ).astype(jnp.bfloat16)
    csend[16:32, :] = parts.astype(jnp.bfloat16)

    others(plane_me, lambda k: c_copy(k).start())
    crecv[plane_me] = csend[...]

    others(line_me, lambda k: b_copy(k).wait_send())
    others(plane_me, lambda k: c_copy(k).wait_send())
    others(plane_me, lambda k: c_arrival(k).wait_recv())
    coef_out[...] = crecv[...]


def combine(coefficients, spectra, modes, energy):
    pick_row = one_hot_rows(192, 64, lambda i: lax.rem(i, 2) * 32 + i // 6)
    row_c = lax.rem(lax.broadcasted_iota(jnp.int32, (192, 192), 0) // 2, 3)
    col_c = lax.broadcasted_iota(jnp.int32, (192, 192), 1) // 64
    same_c = row_c == col_c
    for f in range(STEP):
        message = coefficients[f]
        upper = jnp.concatenate([message[0:16, 0:32], message[0:16, 32:64]], 0)
        lower = jnp.concatenate([message[0:16, 64:96], message[0:16, 96:128]], 0)
        coef = jnp.concatenate(
            [jnp.concatenate([upper, lower], 1), jnp.concatenate([-lower, upper], 1)], 0
        )
        wide = dot_nt(pick_row, coef)
        wide = jnp.where(same_c, jnp.concatenate([wide, wide, wide], 1), 0.0).astype(jnp.bfloat16)
        stacked = spectra[f].reshape(192, LANES)
        modes[f * 192 : (f + 1) * 192, :] = dot_nn(wide, stacked).astype(jnp.bfloat16)
        parts = message[16:32].astype(jnp.float32)
        energy[pl.program_id(0) * STEP + f] = jnp.sum(parts[:, 0:1])


def local(snapshots, block_starts, freq_index):
    xt = jnp.transpose(snapshots, (1, 0, 2))
    dma = pltpu.SemaphoreType.DMA
    vmem = pltpu.VMEM
    bf, f32 = jnp.bfloat16, jnp.float32
    spectra, coefficients = pl.pallas_call(
        kernel,
        out_shape=(
            jax.ShapeDtypeStruct((NF, 3, 64, LANES), bf),
            jax.ShapeDtypeStruct((NF, 32, LANES), bf),
        ),
        in_specs=[
            pl.BlockSpec(memory_space=pl.ANY),
            pl.BlockSpec(memory_space=pltpu.HBM),
            pl.BlockSpec(memory_space=pltpu.HBM),
        ],
        out_specs=(
            pl.BlockSpec(memory_space=pltpu.VMEM),
            pl.BlockSpec(memory_space=pltpu.VMEM),
        ),
        scratch_shapes=[
            pltpu.SMEM((NB,), jnp.int32),
            pltpu.SMEM((NF,), jnp.int32),
            vmem((PEERS, WB * 32, ROWS), bf),
            vmem((3, SLABS, PEERS, ROWS, LANES), bf),
            vmem((LAG + 1, OWN, 32, LANES), f32),
            vmem((3, SLABS, 4, 32, LANES), f32),
            vmem((3, SLABS, 4, 32, LANES), f32),
            vmem((3, SLABS, 128, LANES), bf),
            vmem((3, SLABS, 128, LANES), bf),
            vmem((NF // 2, 128, LANES), f32),
            vmem((NF, 8, LANES), f32),
            vmem((NF, 8, LANES), f32),
            vmem((8, LANES), f32),
            vmem((16, 8, LANES), f32),
            vmem((32, LANES), bf),
            vmem((16, 32, LANES), bf),
            dma((3, SLABS, PEERS)),
            dma((3, SLABS, PEERS)),
            dma((3, SLABS, 4)),
            dma((3, SLABS, 4)),
            dma((3, SLABS)),
            dma((3, SLABS)),
            dma((16,)),
            dma((16,)),
            dma((16,)),
            dma((16,)),
            dma((16,)),
            dma((16,)),
            dma((2,)),
        ],
        compiler_params=pltpu.CompilerParams(
            collective_id=0, has_side_effects=True, vmem_limit_bytes=50 * 2**20
        ),
        name="spectra",
    )(xt, block_starts, freq_index)
    modes, energy = pl.pallas_call(
        combine,
        grid=(NF // STEP,),
        out_shape=(
            jax.ShapeDtypeStruct((NF * 192, LANES), bf),
            jax.ShapeDtypeStruct((NF,), f32),
        ),
        in_specs=[
            pl.BlockSpec((STEP, 32, LANES), lambda i: (i, 0, 0)),
            pl.BlockSpec((STEP, 3, 64, LANES), lambda i: (i, 0, 0, 0)),
        ],
        out_specs=(
            pl.BlockSpec((STEP * 192, LANES), lambda i: (i, 0)),
            pl.BlockSpec(memory_space=pltpu.SMEM),
        ),
        compiler_params=pltpu.CompilerParams(vmem_limit_bytes=50 * 2**20),
        name="modes",
    )(coefficients, spectra)
    modes = modes.reshape(NF, NB, 3, 2, LANES)
    return (jnp.transpose(modes, (0, 1, 3, 2, 4)), energy)


def solution(mesh):
    return jax.shard_map(
        local,
        mesh=mesh,
        in_specs=(P("tm", None, "freq"), P(), P()),
        out_specs=(P(None, None, None, None, ("freq", "tm")), P()),
        check_vma=False,
    )
```

```python
import functools
import math

import jax
import jax.numpy as jnp
from jax import lax
from jax.experimental import pallas as pl
from jax.experimental.pallas import tpu as pltpu
from jax.sharding import PartitionSpec as P

NB = 32
NFFT = 256
NF = 16
NSIT = 6
SLABS = 8
PEERS = 8
ROWS = 68
OWN = 4
WB = 8
UNITS = 3 * SLABS
AHEAD = 6
LAG = 3
HOPS = 4
MAIN = 64
REST = 4
STEP = 16
LANES = 128
POINTS = 32768.0
MESH = pl.DeviceIdType.MESH


def dft_rows(small):
    row = lax.broadcasted_iota(jnp.int32, (2 * NF, NFFT), 0)
    time = lax.broadcasted_iota(jnp.int32, (2 * NF, NFFT), 1)
    bins = jnp.zeros((2 * NF, NFFT), jnp.int32)
    for f in range(NF):
        bins = jnp.where(row // 2 == f, small[NB + f], bins)
    angles = 2.0 * math.pi / NFFT * lax.rem(bins * time, NFFT).astype(jnp.float32)
    window = 0.5 - 0.5 * jnp.cos(2.0 * math.pi / NFFT * time[0:8].astype(jnp.float32))
    scaling = 1.0 / jnp.sqrt(jnp.sum((window * window)[0:1], axis=1, keepdims=True))
    window = jnp.concatenate([window] * (2 * NF // 8), 0)
    wave = jnp.where(lax.rem(row, 2) == 0, window * jnp.cos(angles), -window * jnp.sin(angles))
    return (wave * scaling).astype(jnp.bfloat16)


def one_hot_rows(rows, cols, source):
    i = lax.broadcasted_iota(jnp.int32, (rows, cols), 0)
    j = lax.broadcasted_iota(jnp.int32, (rows, cols), 1)
    return jnp.where(source(i) == j, 1.0, 0.0).astype(jnp.bfloat16)


def dot_nn(a, b, precision=None):
    return lax.dot_general(
        a, b, (((1,), (0,)), ((), ())), precision=precision, preferred_element_type=jnp.float32
    )


def dot_nt(a, b, precision=None):
    return lax.dot_general(
        a, b, (((1,), (1,)), ((), ())), precision=precision, preferred_element_type=jnp.float32
    )


def step_slab(step):
    return lax.rem(step, 2) * 4 + lax.rem(step // 2, 2) * 2 + step // 4


def kernel(
    xt,
    small_hbm,
    sxy,
    coef_out,
    small,
    weights,
    rest_weights,
    rest_stage,
    rest_send,
    rest_recv,
    rbuf,
    own,
    hsend,
    hrecv,
    zsend,
    spec,
    gacc,
    gsend,
    grecv,
    bsend,
    brecv,
    csend,
    crecv,
    ysend_sem,
    yrecv_sem,
    hsend_sem,
    hrecv_sem,
    zsend_sem,
    zrecv_sem,
    gsend_sem,
    grecv_sem,
    bsend_sem,
    brecv_sem,
    csend_sem,
    crecv_sem,
    small_sem,
    news_sem,
    rest_send_sem,
    rest_recv_sem,
):
    tm = lax.axis_index("tm")
    fx = lax.axis_index("freq")
    z = tm // PEERS
    me = lax.rem(tm, PEERS)
    y = me // 2
    core = lax.rem(me, 2)

    def slab_peer(p):
        return {"tm": z * PEERS + p, "freq": fx}

    def column_peer(zz):
        return {"tm": zz * PEERS + me, "freq": fx}

    def plane_peer(k):
        return {"tm": z * PEERS + lax.rem(k, 4) * 2 + core, "freq": k // 4}

    def line_peer(k):
        return {"tm": (k // 2) * PEERS + y * 2 + lax.rem(k, 2), "freq": fx}

    plane_me = fx * 4 + y
    line_me = z * 2 + core

    small_copy = pltpu.make_async_copy(small_hbm, small, small_sem.at[0])
    rest_copy = pltpu.make_async_copy(xt.at[:, pl.ds(MAIN, REST), :], rest_stage, small_sem.at[1])
    rest_copy.start()
    small_copy.start()

    barrier = pltpu.get_barrier_semaphore()

    def around(k):
        zs = lax.rem(z + (SLABS + 1, SLABS - 1, SLABS, SLABS)[k], SLABS)
        xs = lax.rem(fx + (4, 4, 5, 3)[k], 4)
        return {"tm": zs * PEERS + me, "freq": xs}

    def greet(device):
        pl.semaphore_signal(barrier, inc=1, device_id=device, device_id_type=MESH)

    @pl.loop(1, PEERS)
    def _(d):
        greet(slab_peer(lax.rem(me + d, PEERS)))

    for k in range(4):
        greet(around(k))

    def tell(hop):
        for k in range(4):
            pl.semaphore_signal(
                news_sem.at[hop, k], inc=1, device_id=around(k), device_id_type=MESH
            )

    def hear(hop):
        for k in range(4):
            pl.semaphore_wait(news_sem.at[hop, k], 1)

    small_copy.wait()
    table = dft_rows(small)
    rest_copy.wait()
    for c in range(3):
        for zz in range(SLABS):
            for p in range(PEERS):
                col = (zz * PEERS + p) * LANES
                rest_send[p, c, zz * REST : zz * REST + REST, :] = rest_stage[
                    c, :, col : col + LANES
                ]

    pl.semaphore_wait(barrier, 11)
    tell(0)

    def seat(p):
        return pl.ds(pl.multiple_of(p * MAIN, MAIN), MAIN)

    def rest_move(p, source):
        return pltpu.make_async_remote_copy(
            src_ref=rest_send.at[p],
            dst_ref=rest_recv.at[source],
            send_sem=rest_send_sem.at[p],
            recv_sem=rest_recv_sem.at[source],
            device_id=slab_peer(p),
            device_id_type=MESH,
        )

    @pl.loop(1, PEERS)
    def _(d):
        rest_move(lax.rem(me + d, PEERS), me).start()

    def y_copy(c, zz, p):
        cols = pl.ds(pl.multiple_of((zz * PEERS + p) * LANES, LANES), LANES)
        return pltpu.make_async_remote_copy(
            src_ref=xt.at[c, pl.ds(0, MAIN), cols],
            dst_ref=rbuf.at[c, zz, seat(me)],
            send_sem=ysend_sem.at[c, zz, p],
            recv_sem=yrecv_sem.at[c, zz, me],
            device_id=slab_peer(p),
            device_id_type=MESH,
        )

    def y_arrival(c, zz, p):
        return pltpu.make_async_remote_copy(
            src_ref=rbuf.at[c, zz, seat(p)],
            dst_ref=rbuf.at[c, zz, seat(p)],
            send_sem=ysend_sem.at[c, zz, p],
            recv_sem=yrecv_sem.at[c, zz, p],
            device_id=slab_peer(p),
            device_id_type=MESH,
        )

    def y_local(c, zz):
        cols = pl.ds(pl.multiple_of((zz * PEERS + me) * LANES, LANES), LANES)
        return pltpu.make_async_copy(
            xt.at[c, pl.ds(0, MAIN), cols], rbuf.at[c, zz, seat(me)], yrecv_sem.at[c, zz, me]
        )

    def y_start(u):
        c, zz = u // SLABS, step_slab(lax.rem(u, SLABS))

        @pl.loop(1, PEERS)
        def _(d):
            y_copy(c, zz, lax.rem(me + d, PEERS)).start()

        y_local(c, zz).start()

    @pl.loop(0, AHEAD)
    def _(u):
        y_start(u)

    tau = lax.broadcasted_iota(jnp.int32, (NFFT, LANES), 0)
    lane = lax.broadcasted_iota(jnp.int32, (NFFT, LANES), 1)
    lag = tau - (lane // MAIN * ROWS + lax.rem(lane, MAIN))
    rest_lag = tau - (lane // 32 * ROWS + MAIN + lax.rem(lane, REST))

    def placed_rows(lags, value):
        pick = jnp.where(lags == value, 1.0, 0.0).astype(jnp.bfloat16)
        return dot_nn(table, pick).astype(jnp.bfloat16)

    for i in range(WB):
        b = z * OWN - 2 + i
        late = z * (PEERS * ROWS) - small[jnp.clip(b, 0, NB - 1)]
        rows = slice(i * 32, i * 32 + 32)
        for q in range(4):
            weights[rows, q * LANES : (q + 1) * LANES] = placed_rows(lag, late + 2 * q * ROWS)
        for q in range(2):
            rest_weights[rows, q * LANES : (q + 1) * LANES] = placed_rows(
                rest_lag, late + 4 * q * ROWS
            )

    for hop in range(HOPS - 1):
        hear(hop)
        tell(hop + 1)
    hear(HOPS - 1)

    order = one_hot_rows(128, 128, lambda i: lax.rem(i // 2, 4) * 32 + (i // 8) * 2 + lax.rem(i, 2))
    arrange = one_hot_rows(
        128,
        128,
        lambda i: (lax.rem(i, 32) // 4) * 16
        + (i // 64) * 8
        + lax.rem(i, 4) * 2
        + lax.rem(i // 32, 2),
    )

    def h_copy(c, zz, slot, target):
        return pltpu.make_async_remote_copy(
            src_ref=hsend.at[c, zz, slot],
            dst_ref=hrecv.at[c, zz, slot],
            send_sem=hsend_sem.at[c, zz, slot],
            recv_sem=hrecv_sem.at[c, zz, slot],
            device_id=column_peer(target),
            device_id_type=MESH,
        )

    def helpers(c, zz, act_send=None, act_take=None):
        up = jnp.minimum(z + 1, SLABS - 1)
        down = jnp.maximum(z - 1, 0)
        for slot, target, sends, takes in (
            (0, up, z <= 6, z >= 1),
            (1, up, (z >= 4) & (z <= 6), z >= 5),
            (2, down, z == 1, z == 0),
            (3, down, (z >= 1) & (z <= 5), z <= 4),
        ):
            if act_send is not None:

                @pl.when(sends)
                def _():
                    act_send(h_copy(c, zz, slot, target))

            if act_take is not None:

                @pl.when(takes)
                def _():
                    act_take(h_copy(c, zz, slot, target), slot)

    def z_copy(c, zz):
        return pltpu.make_async_remote_copy(
            src_ref=zsend.at[c, zz],
            dst_ref=spec.at[c, z],
            send_sem=zsend_sem.at[c, zz],
            recv_sem=zrecv_sem.at[c, z],
            device_id=column_peer(zz),
            device_id_type=MESH,
        )

    def z_arrival(c, zz):
        return pltpu.make_async_remote_copy(
            src_ref=spec.at[c, zz],
            dst_ref=spec.at[c, zz],
            send_sem=zsend_sem.at[c, zz],
            recv_sem=zrecv_sem.at[c, zz],
            device_id=column_peer(zz),
            device_id_type=MESH,
        )

    rest_lane = lax.broadcasted_iota(jnp.int32, (WB * 32, PEERS * 32), 1)

    def partial(u):
        c, zz, slot = u // SLABS, step_slab(lax.rem(u, SLABS)), lax.rem(u, LAG + 1)
        y_local(c, zz).wait()

        @pl.loop(1, PEERS)
        def _(d):
            y_arrival(c, zz, lax.rem(me + d, PEERS)).wait_recv()

        mine = lax.rem(rest_lane // REST, SLABS) == zz
        chosen = jnp.where(mine, rest_weights[...].astype(jnp.float32), 0.0).astype(jnp.bfloat16)
        acc = dot_nn(weights[...], rbuf[c, zz])
        acc = acc + dot_nn(chosen, rest_recv[:, c].reshape(PEERS * 32, LANES))
        acc = acc.reshape(WB, 32, LANES)
        hsend[c, zz, 2:4] = acc[0:2]
        hsend[c, zz, 0:2] = acc[6:8]
        own[slot] = acc[2:6]
        helpers(c, zz, act_send=lambda copy: copy.start())

    def finish(u):
        c, zz, slot = u // SLABS, step_slab(lax.rem(u, SLABS)), lax.rem(u, LAG + 1)

        def take(copy, i):
            copy.wait_recv()
            own[slot, i] = own[slot, i] + hrecv[c, zz, i]

        helpers(c, zz, act_take=take)
        total = own[slot].astype(jnp.bfloat16).reshape(OWN * 32, LANES)
        rows = dot_nn(order, total).astype(jnp.bfloat16)

        @pl.when(zz == z)
        def _():
            spec[c, z] = rows

        @pl.when(zz != z)
        def _():
            zsend[c, zz] = rows
            z_copy(c, zz).start()

    def pipeline(first, last):
        @pl.loop(first, last)
        def _(u):
            partial(u)

            @pl.when(u + AHEAD < UNITS)
            def _():
                y_start(u + AHEAD)

            @pl.when(u >= LAG)
            def _():
                finish(u - LAG)

    def gather(c):
        @pl.loop(1, SLABS)
        def _(d):
            z_arrival(c, lax.rem(z + d, SLABS)).wait_recv()

        for pair in range(NF // 2):
            stacked = spec[c, :, pl.ds(pair * 16, 16), :].reshape(128, LANES)
            placed = dot_nn(arrange, stacked).astype(jnp.bfloat16)
            sxy[2 * pair, c] = placed[0:64]
            sxy[2 * pair + 1, c] = placed[64:128]
            products = dot_nt(placed, placed)
            if c > 0:
                products = products + gacc[pair]
            if c < 2:
                gacc[pair] = products
            else:
                for h in range(2):
                    k = h * 64
                    xx = products[k : k + 32, k : k + 32]
                    yy = products[k + 32 : k + 64, k + 32 : k + 64]
                    xy = products[k : k + 32, k + 32 : k + 64]
                    yx = products[k + 32 : k + 64, k : k + 32]
                    both = jnp.where(on_or_above, xx + yy, xy - yx)
                    gsend[2 * pair + h] = jnp.concatenate(
                        [both[8 * q : 8 * q + 8] for q in range(4)], 1
                    )

    row32 = lax.broadcasted_iota(jnp.int32, (NB, NB), 0)
    col32 = lax.broadcasted_iota(jnp.int32, (NB, NB), 1)
    on_or_above = col32 >= row32

    rest_recv[me] = rest_send[me]

    @pl.loop(1, PEERS)
    def _(d):
        p = lax.rem(me + d, PEERS)
        rest_move(p, p).wait_recv()
        rest_move(p, p).wait_send()

    pipeline(0, 15)
    gather(0)
    pipeline(15, 23)
    gather(1)
    pipeline(23, UNITS)

    @pl.loop(UNITS - LAG, UNITS)
    def _(u):
        finish(u)

    gather(2)

    def g_copy(k):
        return pltpu.make_async_remote_copy(
            src_ref=gsend.at[k],
            dst_ref=grecv.at[plane_me],
            send_sem=gsend_sem.at[k],
            recv_sem=grecv_sem.at[plane_me],
            device_id=plane_peer(k),
            device_id_type=MESH,
        )

    def g_arrival(k):
        return pltpu.make_async_remote_copy(
            src_ref=grecv.at[k],
            dst_ref=grecv.at[k],
            send_sem=gsend_sem.at[k],
            recv_sem=grecv_sem.at[k],
            device_id=plane_peer(k),
            device_id_type=MESH,
        )

    def b_copy(k):
        return pltpu.make_async_remote_copy(
            src_ref=bsend,
            dst_ref=brecv.at[line_me],
            send_sem=bsend_sem.at[k],
            recv_sem=brecv_sem.at[line_me],
            device_id=line_peer(k),
            device_id_type=MESH,
        )

    def b_arrival(k):
        return pltpu.make_async_remote_copy(
            src_ref=brecv.at[k],
            dst_ref=brecv.at[k],
            send_sem=bsend_sem.at[k],
            recv_sem=brecv_sem.at[k],
            device_id=line_peer(k),
            device_id_type=MESH,
        )

    def c_copy(k):
        return pltpu.make_async_remote_copy(
            src_ref=csend,
            dst_ref=crecv.at[plane_me],
            send_sem=csend_sem.at[k],
            recv_sem=crecv_sem.at[plane_me],
            device_id=plane_peer(k),
            device_id_type=MESH,
        )

    def c_arrival(k):
        return pltpu.make_async_remote_copy(
            src_ref=crecv.at[k],
            dst_ref=crecv.at[k],
            send_sem=csend_sem.at[k],
            recv_sem=crecv_sem.at[k],
            device_id=plane_peer(k),
            device_id_type=MESH,
        )

    def others(mine, act):
        @pl.loop(1, 16)
        def _(d):
            act(lax.rem(mine + d, 16))

    others(plane_me, lambda k: g_copy(k).start())
    grecv[plane_me] = gsend[plane_me]

    @pl.loop(0, UNITS)
    def _(u):
        c, zz = u // SLABS, lax.rem(u, SLABS)

        @pl.loop(1, PEERS)
        def _(d):
            y_copy(c, zz, lax.rem(me + d, PEERS)).wait_send()

    others(plane_me, lambda k: g_arrival(k).wait_recv())
    bsend[...] = jnp.sum(grecv[...], axis=0)

    others(line_me, lambda k: b_copy(k).start())
    brecv[line_me] = bsend[...]

    @pl.loop(0, UNITS)
    def _(u):
        c, zz = u // SLABS, lax.rem(u, SLABS)
        helpers(c, zz, act_send=lambda copy: copy.wait_send())

        @pl.when(zz != z)
        def _():
            z_copy(c, zz).wait_send()

    others(plane_me, lambda k: g_copy(k).wait_send())
    others(line_me, lambda k: b_arrival(k).wait_recv())

    packed = jnp.sum(brecv[...], axis=0)
    both = jnp.concatenate([packed[:, 32 * k : 32 * k + 32] for k in range(4)], 0)
    flipped = both.T
    gram_re = jnp.where(on_or_above, both, flipped)
    gram_im = jnp.where(col32 < row32, both, jnp.where(col32 == row32, 0.0, -flipped))
    hermit = jnp.concatenate(
        [jnp.concatenate([gram_re, -gram_im], 1), jnp.concatenate([gram_im, gram_re], 1)], 0
    )
    row64 = lax.broadcasted_iota(jnp.int32, (64, 64), 0)
    eye = jnp.where(row64 == lax.broadcasted_iota(jnp.int32, (64, 64), 1), 1.0, 0.0)
    square = jnp.sum(jnp.sum(hermit * hermit, axis=1, keepdims=True), axis=0, keepdims=True)
    frob = jnp.sqrt(square + 1e-06)
    trace = jnp.sum(
        jnp.sum(jnp.where(col32 == row32, both, 0.0), axis=1, keepdims=True), axis=0, keepdims=True
    )
    iterate = hermit / frob
    high = lax.Precision.HIGHEST
    factor = 1.5 * eye - 0.5 * iterate
    inverse = factor
    iterate = dot_nn(iterate, factor, high)
    for iteration in range(1, NSIT):
        factor = 1.5 * eye - 0.5 * dot_nn(inverse, iterate, high)
        inverse = dot_nn(factor, inverse, high)
        if iteration < NSIT - 1:
            iterate = dot_nn(iterate, factor, high)
    columns = inverse[:, :NB] * jnp.sqrt(6.0 * POINTS / frob)
    energy = jnp.broadcast_to(trace / (3.0 * NB * POINTS), (16, LANES))
    high_part = energy.astype(jnp.bfloat16).astype(jnp.float32)
    mid_part = (energy - high_part).astype(jnp.bfloat16).astype(jnp.float32)
    low_part = energy - high_part - mid_part
    row16 = lax.broadcasted_iota(jnp.int32, (16, LANES), 0)
    parts = jnp.where(
        row16 == 0, high_part, jnp.where(row16 == 1, mid_part, jnp.where(row16 == 2, low_part, 0.0))
    )
    csend[0:16, :] = jnp.concatenate(
        [columns[16 * q : 16 * q + 16] for q in range(4)], 1
    ).astype(jnp.bfloat16)
    csend[16:32, :] = parts.astype(jnp.bfloat16)

    others(plane_me, lambda k: c_copy(k).start())
    crecv[plane_me] = csend[...]

    others(line_me, lambda k: b_copy(k).wait_send())
    others(plane_me, lambda k: c_copy(k).wait_send())
    others(plane_me, lambda k: c_arrival(k).wait_recv())
    coef_out[...] = crecv[...]


def combine(coefficients, spectra, modes, energy):
    pick_row = one_hot_rows(192, 64, lambda i: lax.rem(i, 2) * 32 + i // 6)
    row_c = lax.rem(lax.broadcasted_iota(jnp.int32, (192, 192), 0) // 2, 3)
    col_c = lax.broadcasted_iota(jnp.int32, (192, 192), 1) // 64
    same_c = row_c == col_c
    for f in range(STEP):
        message = coefficients[f]
        upper = jnp.concatenate([message[0:16, 0:32], message[0:16, 32:64]], 0)
        lower = jnp.concatenate([message[0:16, 64:96], message[0:16, 96:128]], 0)
        coef = jnp.concatenate(
            [jnp.concatenate([upper, lower], 1), jnp.concatenate([-lower, upper], 1)], 0
        )
        wide = dot_nt(pick_row, coef)
        wide = jnp.where(same_c, jnp.concatenate([wide, wide, wide], 1), 0.0).astype(jnp.bfloat16)
        stacked = spectra[f].reshape(192, LANES)
        modes[f * 192 : (f + 1) * 192, :] = dot_nn(wide, stacked).astype(jnp.bfloat16)
        parts = message[16:32].astype(jnp.float32)
        energy[pl.program_id(0) * STEP + f] = jnp.sum(parts[:, 0:1])


def local(snapshots, block_starts, freq_index):
    xt = jnp.transpose(snapshots, (1, 0, 2))
    dma = pltpu.SemaphoreType.DMA
    vmem = pltpu.VMEM
    bf, f32 = jnp.bfloat16, jnp.float32
    spectra, coefficients = pl.pallas_call(
        kernel,
        out_shape=(
            jax.ShapeDtypeStruct((NF, 3, 64, LANES), bf),
            jax.ShapeDtypeStruct((NF, 32, LANES), bf),
        ),
        in_specs=[
            pl.BlockSpec(memory_space=pl.ANY),
            pl.BlockSpec(memory_space=pltpu.HBM),
        ],
        out_specs=(
            pl.BlockSpec(memory_space=pltpu.VMEM),
            pl.BlockSpec(memory_space=pltpu.VMEM),
        ),
        scratch_shapes=[
            pltpu.SMEM((NB + NF,), jnp.int32),
            vmem((WB * 32, PEERS * MAIN), bf),
            vmem((WB * 32, PEERS * 32), bf),
            vmem((3, REST, SLABS * PEERS * LANES), bf),
            vmem((PEERS, 3, 32, LANES), bf),
            vmem((PEERS, 3, 32, LANES), bf),
            vmem((3, SLABS, PEERS * MAIN, LANES), bf),
            vmem((LAG + 1, OWN, 32, LANES), f32),
            vmem((3, SLABS, 4, 32, LANES), f32),
            vmem((3, SLABS, 4, 32, LANES), f32),
            vmem((3, SLABS, 128, LANES), bf),
            vmem((3, SLABS, 128, LANES), bf),
            vmem((NF // 2, 128, LANES), f32),
            vmem((NF, 8, LANES), f32),
            vmem((NF, 8, LANES), f32),
            vmem((8, LANES), f32),
            vmem((16, 8, LANES), f32),
            vmem((32, LANES), bf),
            vmem((16, 32, LANES), bf),
            dma((3, SLABS, PEERS)),
            dma((3, SLABS, PEERS)),
            dma((3, SLABS, 4)),
            dma((3, SLABS, 4)),
            dma((3, SLABS)),
            dma((3, SLABS)),
            dma((16,)),
            dma((16,)),
            dma((16,)),
            dma((16,)),
            dma((16,)),
            dma((16,)),
            dma((2,)),
            pltpu.SemaphoreType.REGULAR((HOPS, 4)),
            dma((PEERS,)),
            dma((PEERS,)),
        ],
        compiler_params=pltpu.CompilerParams(
            collective_id=0, has_side_effects=True, vmem_limit_bytes=50 * 2**20
        ),
        name="spectra",
    )(xt, jnp.concatenate([block_starts, freq_index]))
    modes, energy = pl.pallas_call(
        combine,
        grid=(NF // STEP,),
        out_shape=(
            jax.ShapeDtypeStruct((NF * 192, LANES), bf),
            jax.ShapeDtypeStruct((NF,), f32),
        ),
        in_specs=[
            pl.BlockSpec((STEP, 32, LANES), lambda i: (i, 0, 0)),
            pl.BlockSpec((STEP, 3, 64, LANES), lambda i: (i, 0, 0, 0)),
        ],
        out_specs=(
            pl.BlockSpec((STEP * 192, LANES), lambda i: (i, 0)),
            pl.BlockSpec(memory_space=pltpu.SMEM),
        ),
        compiler_params=pltpu.CompilerParams(vmem_limit_bytes=50 * 2**20),
        name="modes",
    )(coefficients, spectra)
    modes = modes.reshape(NF, NB, 3, 2, LANES)
    return (jnp.transpose(modes, (0, 1, 3, 2, 4)), energy)


def solution(mesh):
    return jax.shard_map(
        local,
        mesh=mesh,
        in_specs=(P("tm", None, "freq"), P(), P()),
        out_specs=(P(None, None, None, None, ("freq", "tm")), P()),
        check_vma=False,
    )
```

```python
import functools
import math

import jax
import jax.numpy as jnp
from jax import lax
from jax.experimental import pallas as pl
from jax.experimental.pallas import tpu as pltpu
from jax.sharding import PartitionSpec as P

NB = 32
NFFT = 256
NF = 16
NSIT = 6
SLABS = 8
PEERS = 8
ROWS = 68
OWN = 4
WB = 8
UNITS = 3 * SLABS
AHEAD = 6
LAG = 3
HOPS = 4
MAIN = 64
REST = 4
STEP = 16
LANES = 128
POINTS = 32768.0
MESH = pl.DeviceIdType.MESH


def dft_rows(small):
    row = lax.broadcasted_iota(jnp.int32, (2 * NF, NFFT), 0)
    time = lax.broadcasted_iota(jnp.int32, (2 * NF, NFFT), 1)
    bins = jnp.zeros((2 * NF, NFFT), jnp.int32)
    for f in range(NF):
        bins = jnp.where(row // 2 == f, small[NB + f], bins)
    angles = 2.0 * math.pi / NFFT * lax.rem(bins * time, NFFT).astype(jnp.float32)
    window = 0.5 - 0.5 * jnp.cos(2.0 * math.pi / NFFT * time[0:8].astype(jnp.float32))
    scaling = 1.0 / jnp.sqrt(jnp.sum((window * window)[0:1], axis=1, keepdims=True))
    window = jnp.concatenate([window] * (2 * NF // 8), 0)
    wave = jnp.where(lax.rem(row, 2) == 0, window * jnp.cos(angles), -window * jnp.sin(angles))
    return (wave * scaling).astype(jnp.bfloat16)


def one_hot_rows(rows, cols, source):
    i = lax.broadcasted_iota(jnp.int32, (rows, cols), 0)
    j = lax.broadcasted_iota(jnp.int32, (rows, cols), 1)
    return jnp.where(source(i) == j, 1.0, 0.0).astype(jnp.bfloat16)


def dot_nn(a, b, precision=None):
    return lax.dot_general(
        a, b, (((1,), (0,)), ((), ())), precision=precision, preferred_element_type=jnp.float32
    )


def dot_nt(a, b, precision=None):
    return lax.dot_general(
        a, b, (((1,), (1,)), ((), ())), precision=precision, preferred_element_type=jnp.float32
    )


def step_slab(step):
    return lax.rem(step, 2) * 4 + lax.rem(step // 2, 2) * 2 + step // 4


def kernel(
    xt,
    small_hbm,
    sxy,
    coef_out,
    small,
    weights,
    rest_weights,
    rest_stage,
    rest_send,
    rest_recv,
    rbuf,
    own,
    hsend,
    hrecv,
    zsend,
    spec,
    gacc,
    gsend,
    grecv,
    bsend,
    brecv,
    csend,
    crecv,
    ysend_sem,
    yrecv_sem,
    hsend_sem,
    hrecv_sem,
    zsend_sem,
    zrecv_sem,
    gsend_sem,
    grecv_sem,
    bsend_sem,
    brecv_sem,
    csend_sem,
    crecv_sem,
    small_sem,
    news_sem,
    rest_send_sem,
    rest_recv_sem,
):
    tm = lax.axis_index("tm")
    fx = lax.axis_index("freq")
    z = tm // PEERS
    me = lax.rem(tm, PEERS)
    y = me // 2
    core = lax.rem(me, 2)

    def slab_peer(p):
        return {"tm": z * PEERS + p, "freq": fx}

    def column_peer(zz):
        return {"tm": zz * PEERS + me, "freq": fx}

    def plane_peer(k):
        return {"tm": z * PEERS + lax.rem(k, 4) * 2 + core, "freq": k // 4}

    def line_peer(k):
        return {"tm": (k // 2) * PEERS + y * 2 + lax.rem(k, 2), "freq": fx}

    plane_me = fx * 4 + y
    line_me = z * 2 + core

    small_copy = pltpu.make_async_copy(small_hbm, small, small_sem.at[0])
    rest_copy = pltpu.make_async_copy(xt.at[:, pl.ds(MAIN, REST), :], rest_stage, small_sem.at[1])
    rest_copy.start()
    small_copy.start()

    barrier = pltpu.get_barrier_semaphore()

    def around(k):
        zs = lax.rem(z + (SLABS + 1, SLABS - 1, SLABS, SLABS)[k], SLABS)
        xs = lax.rem(fx + (4, 4, 5, 3)[k], 4)
        return {"tm": zs * PEERS + me, "freq": xs}

    def greet(device):
        pl.semaphore_signal(barrier, inc=1, device_id=device, device_id_type=MESH)

    @pl.loop(1, PEERS)
    def _(d):
        greet(slab_peer(lax.rem(me + d, PEERS)))

    for k in range(4):
        greet(around(k))

    def tell(hop):
        for k in range(4):
            pl.semaphore_signal(
                news_sem.at[hop, k], inc=1, device_id=around(k), device_id_type=MESH
            )

    def hear(hop):
        for k in range(4):
            pl.semaphore_wait(news_sem.at[hop, k], 1)

    small_copy.wait()
    table = dft_rows(small)
    rest_copy.wait()
    for c in range(3):
        for zz in range(SLABS):
            for p in range(PEERS):
                col = (zz * PEERS + p) * LANES
                rest_send[p, c, zz * REST : zz * REST + REST, :] = rest_stage[
                    c, :, col : col + LANES
                ]

    pl.semaphore_wait(barrier, 11)
    tell(0)

    def seat(p):
        return pl.ds(pl.multiple_of(p * MAIN, MAIN), MAIN)

    def rest_move(p, source):
        return pltpu.make_async_remote_copy(
            src_ref=rest_send.at[p],
            dst_ref=rest_recv.at[source],
            send_sem=rest_send_sem.at[p],
            recv_sem=rest_recv_sem.at[source],
            device_id=slab_peer(p),
            device_id_type=MESH,
        )

    @pl.loop(1, PEERS)
    def _(d):
        rest_move(lax.rem(me + d, PEERS), me).start()

    def y_copy(c, zz, p):
        cols = pl.ds(pl.multiple_of((zz * PEERS + p) * LANES, LANES), LANES)
        return pltpu.make_async_remote_copy(
            src_ref=xt.at[c, pl.ds(0, MAIN), cols],
            dst_ref=rbuf.at[c, zz, seat(me)],
            send_sem=ysend_sem.at[c, zz, p],
            recv_sem=yrecv_sem.at[c, zz, me],
            device_id=slab_peer(p),
            device_id_type=MESH,
        )

    def y_arrival(c, zz, p):
        return pltpu.make_async_remote_copy(
            src_ref=rbuf.at[c, zz, seat(p)],
            dst_ref=rbuf.at[c, zz, seat(p)],
            send_sem=ysend_sem.at[c, zz, p],
            recv_sem=yrecv_sem.at[c, zz, p],
            device_id=slab_peer(p),
            device_id_type=MESH,
        )

    def y_local(c, zz):
        cols = pl.ds(pl.multiple_of((zz * PEERS + me) * LANES, LANES), LANES)
        return pltpu.make_async_copy(
            xt.at[c, pl.ds(0, MAIN), cols], rbuf.at[c, zz, seat(me)], yrecv_sem.at[c, zz, me]
        )

    def y_start(u):
        c, zz = u // SLABS, step_slab(lax.rem(u, SLABS))

        @pl.loop(1, PEERS)
        def _(d):
            y_copy(c, zz, lax.rem(me + d, PEERS)).start()

        y_local(c, zz).start()

    @pl.loop(0, AHEAD)
    def _(u):
        y_start(u)

    tau = lax.broadcasted_iota(jnp.int32, (NFFT, LANES), 0)
    lane = lax.broadcasted_iota(jnp.int32, (NFFT, LANES), 1)
    lag = tau - (lane // MAIN * ROWS + lax.rem(lane, MAIN))
    rest_lag = tau - (lane // 32 * ROWS + MAIN + lax.rem(lane, REST))

    def placed_rows(lags, value):
        pick = jnp.where(lags == value, 1.0, 0.0).astype(jnp.bfloat16)
        return dot_nn(table, pick).astype(jnp.bfloat16)

    for i in range(WB):
        b = z * OWN - 2 + i
        late = z * (PEERS * ROWS) - small[jnp.clip(b, 0, NB - 1)]
        rows = slice(i * 32, i * 32 + 32)
        for q in range(4):
            weights[rows, q * LANES : (q + 1) * LANES] = placed_rows(lag, late + 2 * q * ROWS)
        for q in range(2):
            rest_weights[rows, q * LANES : (q + 1) * LANES] = placed_rows(
                rest_lag, late + 4 * q * ROWS
            )

    for hop in range(HOPS - 1):
        hear(hop)
        tell(hop + 1)
    hear(HOPS - 1)

    order = one_hot_rows(128, 128, lambda i: lax.rem(i // 2, 4) * 32 + (i // 8) * 2 + lax.rem(i, 2))
    arrange = one_hot_rows(
        128,
        128,
        lambda i: (lax.rem(i, 32) // 4) * 16
        + (i // 64) * 8
        + lax.rem(i, 4) * 2
        + lax.rem(i // 32, 2),
    )

    def h_copy(c, zz, slot, target):
        return pltpu.make_async_remote_copy(
            src_ref=hsend.at[c, zz, slot],
            dst_ref=hrecv.at[c, zz, slot],
            send_sem=hsend_sem.at[c, zz, slot],
            recv_sem=hrecv_sem.at[c, zz, slot],
            device_id=column_peer(target),
            device_id_type=MESH,
        )

    def helpers(c, zz, act_send=None, act_take=None):
        up = jnp.minimum(z + 1, SLABS - 1)
        down = jnp.maximum(z - 1, 0)
        for slot, target, sends, takes in (
            (0, up, z <= 6, z >= 1),
            (1, up, (z >= 4) & (z <= 6), z >= 5),
            (2, down, z == 1, z == 0),
            (3, down, (z >= 1) & (z <= 5), z <= 4),
        ):
            if act_send is not None:

                @pl.when(sends)
                def _():
                    act_send(h_copy(c, zz, slot, target))

            if act_take is not None:

                @pl.when(takes)
                def _():
                    act_take(h_copy(c, zz, slot, target), slot)

    def z_copy(c, zz):
        return pltpu.make_async_remote_copy(
            src_ref=zsend.at[c, zz],
            dst_ref=spec.at[c, z],
            send_sem=zsend_sem.at[c, zz],
            recv_sem=zrecv_sem.at[c, z],
            device_id=column_peer(zz),
            device_id_type=MESH,
        )

    def z_arrival(c, zz):
        return pltpu.make_async_remote_copy(
            src_ref=spec.at[c, zz],
            dst_ref=spec.at[c, zz],
            send_sem=zsend_sem.at[c, zz],
            recv_sem=zrecv_sem.at[c, zz],
            device_id=column_peer(zz),
            device_id_type=MESH,
        )

    rest_lane = lax.broadcasted_iota(jnp.int32, (WB * 32, PEERS * 32), 1)

    def partial(u):
        c, zz, slot = u // SLABS, step_slab(lax.rem(u, SLABS)), lax.rem(u, LAG + 1)
        y_local(c, zz).wait()

        @pl.loop(1, PEERS)
        def _(d):
            y_arrival(c, zz, lax.rem(me + d, PEERS)).wait_recv()

        mine = lax.rem(rest_lane // REST, SLABS) == zz
        chosen = jnp.where(mine, rest_weights[...].astype(jnp.float32), 0.0).astype(jnp.bfloat16)
        acc = dot_nn(weights[...], rbuf[c, zz])
        acc = acc + dot_nn(chosen, rest_recv[:, c].reshape(PEERS * 32, LANES))
        acc = acc.reshape(WB, 32, LANES)
        hsend[c, zz, 2:4] = acc[0:2]
        hsend[c, zz, 0:2] = acc[6:8]
        own[slot] = acc[2:6]
        helpers(c, zz, act_send=lambda copy: copy.start())

    def finish(u):
        c, zz, slot = u // SLABS, step_slab(lax.rem(u, SLABS)), lax.rem(u, LAG + 1)

        def take(copy, i):
            copy.wait_recv()
            own[slot, i] = own[slot, i] + hrecv[c, zz, i]

        helpers(c, zz, act_take=take)
        total = own[slot].astype(jnp.bfloat16).reshape(OWN * 32, LANES)
        rows = dot_nn(order, total).astype(jnp.bfloat16)

        @pl.when(zz == z)
        def _():
            spec[c, z] = rows

        @pl.when(zz != z)
        def _():
            zsend[c, zz] = rows
            z_copy(c, zz).start()

    def pipeline(first, last):
        @pl.loop(first, last)
        def _(u):
            partial(u)

            @pl.when(u + AHEAD < UNITS)
            def _():
                y_start(u + AHEAD)

            @pl.when(u >= LAG)
            def _():
                finish(u - LAG)

    def gather(c):
        @pl.loop(1, SLABS)
        def _(d):
            z_arrival(c, lax.rem(z + d, SLABS)).wait_recv()

        for pair in range(NF // 2):
            stacked = spec[c, :, pl.ds(pair * 16, 16), :].reshape(128, LANES)
            placed = dot_nn(arrange, stacked).astype(jnp.bfloat16)
            sxy[2 * pair, c] = placed[0:64]
            sxy[2 * pair + 1, c] = placed[64:128]
            products = dot_nt(placed, placed)
            if c > 0:
                products = products + gacc[pair]
            if c < 2:
                gacc[pair] = products
            else:
                for h in range(2):
                    k = h * 64
                    xx = products[k : k + 32, k : k + 32]
                    yy = products[k + 32 : k + 64, k + 32 : k + 64]
                    xy = products[k : k + 32, k + 32 : k + 64]
                    yx = products[k + 32 : k + 64, k : k + 32]
                    both = jnp.where(on_or_above, xx + yy, xy - yx)
                    gsend[2 * pair + h] = jnp.concatenate(
                        [both[8 * q : 8 * q + 8] for q in range(4)], 1
                    )

    row32 = lax.broadcasted_iota(jnp.int32, (NB, NB), 0)
    col32 = lax.broadcasted_iota(jnp.int32, (NB, NB), 1)
    on_or_above = col32 >= row32

    rest_recv[me] = rest_send[me]

    @pl.loop(1, PEERS)
    def _(d):
        p = lax.rem(me + d, PEERS)
        rest_move(p, p).wait_recv()
        rest_move(p, p).wait_send()

    pipeline(0, 15)
    gather(0)
    pipeline(15, 23)
    gather(1)
    pipeline(23, UNITS)

    @pl.loop(UNITS - LAG, UNITS)
    def _(u):
        finish(u)

    gather(2)

    def g_copy(k):
        return pltpu.make_async_remote_copy(
            src_ref=gsend.at[k],
            dst_ref=grecv.at[plane_me],
            send_sem=gsend_sem.at[k],
            recv_sem=grecv_sem.at[plane_me],
            device_id=plane_peer(k),
            device_id_type=MESH,
        )

    def g_arrival(k):
        return pltpu.make_async_remote_copy(
            src_ref=grecv.at[k],
            dst_ref=grecv.at[k],
            send_sem=gsend_sem.at[k],
            recv_sem=grecv_sem.at[k],
            device_id=plane_peer(k),
            device_id_type=MESH,
        )

    def b_copy(k):
        return pltpu.make_async_remote_copy(
            src_ref=bsend,
            dst_ref=brecv.at[line_me],
            send_sem=bsend_sem.at[k],
            recv_sem=brecv_sem.at[line_me],
            device_id=line_peer(k),
            device_id_type=MESH,
        )

    def b_arrival(k):
        return pltpu.make_async_remote_copy(
            src_ref=brecv.at[k],
            dst_ref=brecv.at[k],
            send_sem=bsend_sem.at[k],
            recv_sem=brecv_sem.at[k],
            device_id=line_peer(k),
            device_id_type=MESH,
        )

    def c_copy(k):
        return pltpu.make_async_remote_copy(
            src_ref=csend,
            dst_ref=crecv.at[plane_me],
            send_sem=csend_sem.at[k],
            recv_sem=crecv_sem.at[plane_me],
            device_id=plane_peer(k),
            device_id_type=MESH,
        )

    def c_arrival(k):
        return pltpu.make_async_remote_copy(
            src_ref=crecv.at[k],
            dst_ref=crecv.at[k],
            send_sem=csend_sem.at[k],
            recv_sem=crecv_sem.at[k],
            device_id=plane_peer(k),
            device_id_type=MESH,
        )

    def others(mine, act):
        @pl.loop(1, 16)
        def _(d):
            act(lax.rem(mine + d, 16))

    others(plane_me, lambda k: g_copy(k).start())
    grecv[plane_me] = gsend[plane_me]

    @pl.loop(0, UNITS)
    def _(u):
        c, zz = u // SLABS, lax.rem(u, SLABS)

        @pl.loop(1, PEERS)
        def _(d):
            y_copy(c, zz, lax.rem(me + d, PEERS)).wait_send()

    others(plane_me, lambda k: g_arrival(k).wait_recv())
    bsend[...] = jnp.sum(grecv[...], axis=0)

    others(line_me, lambda k: b_copy(k).start())
    brecv[line_me] = bsend[...]

    @pl.loop(0, UNITS)
    def _(u):
        c, zz = u // SLABS, lax.rem(u, SLABS)
        helpers(c, zz, act_send=lambda copy: copy.wait_send())

        @pl.when(zz != z)
        def _():
            z_copy(c, zz).wait_send()

    others(plane_me, lambda k: g_copy(k).wait_send())
    others(line_me, lambda k: b_arrival(k).wait_recv())

    packed = jnp.sum(brecv[...], axis=0)
    both = jnp.concatenate([packed[:, 32 * k : 32 * k + 32] for k in range(4)], 0)
    flipped = both.T
    gram_re = jnp.where(on_or_above, both, flipped)
    gram_im = jnp.where(col32 < row32, both, jnp.where(col32 == row32, 0.0, -flipped))
    hermit = jnp.concatenate(
        [jnp.concatenate([gram_re, -gram_im], 1), jnp.concatenate([gram_im, gram_re], 1)], 0
    )
    row64 = lax.broadcasted_iota(jnp.int32, (64, 64), 0)
    eye = jnp.where(row64 == lax.broadcasted_iota(jnp.int32, (64, 64), 1), 1.0, 0.0)
    square = jnp.sum(jnp.sum(hermit * hermit, axis=1, keepdims=True), axis=0, keepdims=True)
    frob = jnp.sqrt(square + 1e-06)
    trace = jnp.sum(
        jnp.sum(jnp.where(col32 == row32, both, 0.0), axis=1, keepdims=True), axis=0, keepdims=True
    )
    iterate = hermit / frob
    high = lax.Precision.HIGHEST
    factor = 1.5 * eye - 0.5 * iterate
    inverse = factor
    iterate = dot_nn(iterate, factor, high)
    for iteration in range(1, NSIT):
        factor = 1.5 * eye - 0.5 * dot_nn(inverse, iterate, high)
        inverse = dot_nn(factor, inverse, high)
        if iteration < NSIT - 1:
            iterate = dot_nn(iterate, factor, high)
    columns = inverse[:, :NB] * jnp.sqrt(6.0 * POINTS / frob)
    energy = jnp.broadcast_to(trace / (3.0 * NB * POINTS), (16, LANES))
    high_part = energy.astype(jnp.bfloat16).astype(jnp.float32)
    mid_part = (energy - high_part).astype(jnp.bfloat16).astype(jnp.float32)
    low_part = energy - high_part - mid_part
    row16 = lax.broadcasted_iota(jnp.int32, (16, LANES), 0)
    parts = jnp.where(
        row16 == 0, high_part, jnp.where(row16 == 1, mid_part, jnp.where(row16 == 2, low_part, 0.0))
    )
    csend[0:16, :] = jnp.concatenate(
        [columns[16 * q : 16 * q + 16] for q in range(4)], 1
    ).astype(jnp.bfloat16)
    csend[16:32, :] = parts.astype(jnp.bfloat16)

    others(plane_me, lambda k: c_copy(k).start())
    crecv[plane_me] = csend[...]

    others(line_me, lambda k: b_copy(k).wait_send())
    others(plane_me, lambda k: c_copy(k).wait_send())
    others(plane_me, lambda k: c_arrival(k).wait_recv())
    coef_out[...] = crecv[...]


def combine(coefficients, spectra, modes, energy):
    pick_row = one_hot_rows(192, 64, lambda i: lax.rem(i, 2) * 32 + i // 6)
    row_c = lax.rem(lax.broadcasted_iota(jnp.int32, (192, 192), 0) // 2, 3)
    col_c = lax.broadcasted_iota(jnp.int32, (192, 192), 1) // 64
    same_c = row_c == col_c
    for f in range(STEP):
        message = coefficients[f]
        upper = jnp.concatenate([message[0:16, 0:32], message[0:16, 32:64]], 0)
        lower = jnp.concatenate([message[0:16, 64:96], message[0:16, 96:128]], 0)
        coef = jnp.concatenate(
            [jnp.concatenate([upper, lower], 1), jnp.concatenate([-lower, upper], 1)], 0
        )
        wide = dot_nt(pick_row, jnp.concatenate([coef, coef, coef], 0))
        wide = jnp.where(same_c, wide, 0.0).astype(jnp.bfloat16)
        stacked = spectra[f].reshape(192, LANES)
        modes[f * 192 : (f + 1) * 192, :] = dot_nn(wide, stacked).astype(jnp.bfloat16)
        parts = message[16:32].astype(jnp.float32)
        energy[pl.program_id(0) * STEP + f] = jnp.sum(parts[:, 0:1])


def local(snapshots, block_starts, freq_index):
    xt = jnp.transpose(snapshots, (1, 0, 2))
    dma = pltpu.SemaphoreType.DMA
    vmem = pltpu.VMEM
    bf, f32 = jnp.bfloat16, jnp.float32
    spectra, coefficients = pl.pallas_call(
        kernel,
        out_shape=(
            jax.ShapeDtypeStruct((NF, 3, 64, LANES), bf),
            jax.ShapeDtypeStruct((NF, 32, LANES), bf),
        ),
        in_specs=[
            pl.BlockSpec(memory_space=pl.ANY),
            pl.BlockSpec(memory_space=pltpu.HBM),
        ],
        out_specs=(
            pl.BlockSpec(memory_space=pltpu.VMEM),
            pl.BlockSpec(memory_space=pltpu.VMEM),
        ),
        scratch_shapes=[
            pltpu.SMEM((NB + NF,), jnp.int32),
            vmem((WB * 32, PEERS * MAIN), bf),
            vmem((WB * 32, PEERS * 32), bf),
            vmem((3, REST, SLABS * PEERS * LANES), bf),
            vmem((PEERS, 3, 32, LANES), bf),
            vmem((PEERS, 3, 32, LANES), bf),
            vmem((3, SLABS, PEERS * MAIN, LANES), bf),
            vmem((LAG + 1, OWN, 32, LANES), f32),
            vmem((3, SLABS, 4, 32, LANES), f32),
            vmem((3, SLABS, 4, 32, LANES), f32),
            vmem((3, SLABS, 128, LANES), bf),
            vmem((3, SLABS, 128, LANES), bf),
            vmem((NF // 2, 128, LANES), f32),
            vmem((NF, 8, LANES), f32),
            vmem((NF, 8, LANES), f32),
            vmem((8, LANES), f32),
            vmem((16, 8, LANES), f32),
            vmem((32, LANES), bf),
            vmem((16, 32, LANES), bf),
            dma((3, SLABS, PEERS)),
            dma((3, SLABS, PEERS)),
            dma((3, SLABS, 4)),
            dma((3, SLABS, 4)),
            dma((3, SLABS)),
            dma((3, SLABS)),
            dma((16,)),
            dma((16,)),
            dma((16,)),
            dma((16,)),
            dma((16,)),
            dma((16,)),
            dma((2,)),
            pltpu.SemaphoreType.REGULAR((HOPS, 4)),
            dma((PEERS,)),
            dma((PEERS,)),
        ],
        compiler_params=pltpu.CompilerParams(
            collective_id=0, has_side_effects=True, vmem_limit_bytes=50 * 2**20
        ),
        name="spectra",
    )(xt, jnp.concatenate([block_starts, freq_index]))
    modes, energy = pl.pallas_call(
        combine,
        grid=(NF // STEP,),
        out_shape=(
            jax.ShapeDtypeStruct((NF * 192, LANES), bf),
            jax.ShapeDtypeStruct((NF,), f32),
        ),
        in_specs=[
            pl.BlockSpec((STEP, 32, LANES), lambda i: (i, 0, 0)),
            pl.BlockSpec((STEP, 3, 64, LANES), lambda i: (i, 0, 0, 0)),
        ],
        out_specs=(
            pl.BlockSpec((STEP * 192, LANES), lambda i: (i, 0)),
            pl.BlockSpec(memory_space=pltpu.SMEM),
        ),
        compiler_params=pltpu.CompilerParams(vmem_limit_bytes=50 * 2**20),
        name="modes",
    )(coefficients, spectra)
    modes = modes.reshape(NF, NB, 3, 2, LANES)
    return (jnp.transpose(modes, (0, 1, 3, 2, 4)), energy)


def solution(mesh):
    return jax.shard_map(
        local,
        mesh=mesh,
        in_specs=(P("tm", None, "freq"), P(), P()),
        out_specs=(P(None, None, None, None, ("freq", "tm")), P()),
        check_vma=False,
    )
```
